1024 devices in a mesh: ep: 16 (over x_lo, y), grp: 64 (over x_hi, z, core).
Axes of the slice: x: 8 (x_hi: 4, x_lo: 2; x = x_hi * 2 + x_lo), y: 8, z: 8, core: 2. Of those that a mesh axis runs over, the one named last changes fastest.
Arguments:
- tokens: bfloat16 [131072, 4096], P(('ep', 'grp')), may hold values from -6 to 6
- expert_ids: int32 [131072, 8], P(('ep', 'grp')), may hold values from 0 to 127, all different within a row; in each aligned block of 128 rows (0 to 127, 128 to 255, ...) at most 16 rows name the same one
- combine: float32 [131072, 8], P(('ep', 'grp')), may hold values from 0.05 to 1
- w_gate: bfloat16 [4096, 5120], P(None, 'ep'), may hold values from -0.09375 to 0.09375
- w_up: bfloat16 [4096, 5120], P(None, 'ep'), may hold values from -0.09375 to 0.09375
- w_down: bfloat16 [5120, 4096], P('ep'), may hold values from -0.15625 to 0.15625
- bias: float32 [128], replicated, may hold values from -3 to 3
Outputs:
- mixed: bfloat16 [131072, 4096], P(('ep', 'grp'))
- new_bias: float32 [128], replicated
The draws below stay inside these ranges and needn't reach their ends.
Inputs may be any that keep to these rules, and one draw needn't show every extreme that they name: `expert_ids`: each row names 8 different experts. Among the rows of one device no expert is named more than 16 times, a bound that some block reaches.
All inputs are finite; a program needn't handle non-finite values.
Results may differ from the reference program's by a relative error of at most 0.0057.
Values may be sent and summed in bfloat16 or wider, within the bound.
A program may use at most 32 MiB of HBM per device.

```python
import math
import jax
import jax.numpy as jnp
import numpy as np
from jax import lax

D = 4096
NEXP = 128
TOPK = 8
FF_WIN = 1280
SPLIT = 4
TOK_DEV = 128
CAP = 16
FF_DEV = 320
E_WIN = 4
TOKENS = 131072


def block_scale(own_key, extent, split, low, high):
    factor_of, own = 1.0, jax.random.fold_in(own_key, 6)
    for axis_at, parts in split:
        heights = jnp.exp(jax.random.uniform(jax.random.fold_in(own, axis_at), (parts,), jnp.float32, low / len(split), high / len(split)))
        factor_of = factor_of * jnp.repeat(heights, extent[axis_at] // parts).reshape([-1 if axis == axis_at else 1 for axis in range(len(extent))])
    return factor_of


def routed_block(stream_key, own, number, rows, count, top, reach, skew):
    order = jax.random.permutation(stream_key, count)
    packed, ordinary = shares(count, rows * top, reach, skew, True), shares(count, rows * top, reach, skew, False)
    places = jnp.arange(count)

    def named(tallies, turn):
        used = int((tallies > 0).sum())
        fixed = max(1, used // 4)
        passed = fixed + (places - fixed + turn * (used - fixed)) % max(1, count - fixed)
        return jnp.zeros((count,), jnp.int32).at[order[jnp.where(places < fixed, places, passed)]].set(jnp.asarray(tallies, jnp.int32))

    tallies = jnp.where(number % 4 == 0, named(packed, number // 4), named(ordinary, number - number // 4 - 1))
    mixed = jax.random.permutation(jax.random.fold_in(own, 3), count)
    source_of, sink = mixed[0:count // 2 * 2:2], mixed[1:count // 2 * 2:2]
    slack = jnp.minimum(tallies[source_of] - 1, reach - tallies[sink]) // 2
    slack = jnp.where((source_of == order[0]) | (sink == order[0]) | (tallies[sink] == 0), 0, jnp.maximum(slack, 0))
    passed = jax.random.randint(jax.random.fold_in(own, 4), (count // 2,), 0, 1 << 20) % (slack + 1)
    tallies = tallies.at[source_of].add(-passed).at[sink].add(passed)
    members = jnp.searchsorted(jnp.cumsum(tallies), jnp.arange(rows * top), side="right").astype(jnp.int32)
    listing = members.reshape(top, rows).T
    listing = listing[jax.random.permutation(jax.random.fold_in(own, 1), rows)]
    turn = jax.random.randint(jax.random.fold_in(own, 2), (rows, 1), 0, top)
    return jnp.take_along_axis(listing, (jnp.arange(top)[None, :] + turn) % top, axis=1)


def shares(amount, total, reach, lean, full):
    weights = [(1 << 20) // math.isqrt(standing ** lean) + 1 for standing in range(1, amount + 1)]
    largest = reach if full else min(reach, max(-(-total // amount), total * weights[0] // sum(weights)))
    least = 1 if total - largest >= amount - 1 else 0
    counts, rest = [largest] + [least] * (amount - 1), total - largest - least * (amount - 1)
    while rest > 0:
        free = [i for i in range(1, amount) if counts[i] < largest] or [i for i in range(1, amount) if counts[i] < reach]
        pool, remaining = sum([weights[i] for i in free]), rest
        for i in free:
            addition = min(reach - counts[i], max(1, remaining * weights[i] // pool), rest)
            counts[i] = counts[i] + addition
            rest = rest - addition
    return np.array(counts)


def noise(own_key, dims, deviation, most, pieces=(), kind=jnp.bfloat16):
    gain = block_scale(own_key, dims, pieces, -0.22, 0.18) if pieces else 1.0
    entries = jax.random.normal(own_key, dims, jnp.float32) * deviation * gain
    return jnp.minimum(jnp.maximum(entries, -most), most).astype(kind)


def setup_inputs(seed: int = 0) -> dict:
    arg_keys = jax.random.split(jax.random.key(seed), 8)
    tokens = noise(arg_keys[0], (TOKENS, D), 1.0, 6.0, ((0, 1024),))
    expert_ids_keys = jax.random.split(jax.random.fold_in(arg_keys[1], 1), TOKENS // TOK_DEV)
    expert_ids_turns = jax.random.permutation(jax.random.fold_in(arg_keys[1], 3), TOKENS // TOK_DEV)
    expert_ids = jax.vmap(lambda own, number: routed_block(jax.random.fold_in(arg_keys[1], 2), own, number, TOK_DEV, NEXP, TOPK, CAP, 2))(expert_ids_keys, expert_ids_turns).reshape((TOKENS, TOPK))
    combine = jnp.clip(jnp.exp(math.log(1.0) - 2.9957323 * jax.random.uniform(arg_keys[2], (TOKENS, TOPK), jnp.float32) ** block_scale(arg_keys[2], (TOKENS, TOPK), ((0, 1024),), -0.2, 0.2)), 0.05, 1.0)
    w_gate = noise(arg_keys[3], (D, E_WIN * FF_WIN), D ** -0.5, 0.09375, ((1, 16),))
    w_up = noise(arg_keys[4], (D, E_WIN * FF_WIN), D ** -0.5, 0.09375, ((1, 16),))
    w_down = noise(arg_keys[5], (E_WIN * FF_WIN, D), FF_WIN ** -0.5, 0.15625, ((0, 16),))
    bias = noise(arg_keys[6], (NEXP,), 0.5, 3.0, (), jnp.float32)
    return {"tokens": tokens, "expert_ids": expert_ids, "combine": combine, "w_gate": w_gate, "w_up": w_up, "w_down": w_down, "bias": bias}


def reference(tokens, expert_ids, combine, w_gate, w_up, w_down, bias):
    blocks = tokens.shape[0] // TOK_DEV
    picks = expert_ids.reshape(blocks, TOK_DEV * TOPK)
    window = jnp.arange(E_WIN, dtype=jnp.int32)
    hit = (picks[:, :, None] == window[None, None, :]).astype(jnp.int32)
    ranks = jnp.cumsum(hit, axis=1) - 1
    slot = lax.optimization_barrier(jnp.sum(hit * ranks, axis=2))
    inside = lax.optimization_barrier(jnp.sum(hit, axis=2))
    block_idx = jnp.arange(blocks, dtype=jnp.int32)[:, None]
    total_slots = E_WIN * blocks * CAP
    dest = jnp.where(inside > 0, (picks * blocks + block_idx) * CAP + slot, total_slots).reshape(-1).astype(jnp.int32)
    token_of = (jnp.arange(blocks * TOK_DEV * TOPK, dtype=jnp.int32) // TOPK).astype(jnp.int32)
    source = jnp.full((total_slots + 1,), tokens.shape[0], jnp.int32).at[dest].set(token_of)[:total_slots]
    weight = jnp.zeros((total_slots + 1,), jnp.float32).at[dest].set(combine.reshape(-1).astype(jnp.float32))[:total_slots]
    padded = jnp.concatenate([tokens, jnp.zeros((1, tokens.shape[1]), tokens.dtype)], axis=0)
    rows_all = padded[source].reshape(E_WIN, blocks * CAP, tokens.shape[1])

    def expert(index):
        rows = rows_all[index]
        total = jnp.zeros((rows.shape[0], tokens.shape[1]), jnp.float32)
        for piece in range(SPLIT):
            start = index * FF_WIN + piece * FF_DEV
            g_cols = lax.dynamic_slice_in_dim(w_gate, start, FF_DEV, 1)
            u_cols = lax.dynamic_slice_in_dim(w_up, start, FF_DEV, 1)
            d_rows = lax.dynamic_slice_in_dim(w_down, start, FF_DEV, 0)
            gate = jnp.dot(rows, g_cols, preferred_element_type=jnp.float32)
            upval = jnp.dot(rows, u_cols, preferred_element_type=jnp.float32)
            hidden = (jax.nn.silu(gate) * upval).astype(jnp.bfloat16)
            part = jnp.dot(hidden, d_rows, preferred_element_type=jnp.float32).astype(jnp.bfloat16)
            total = total + part.astype(jnp.float32)
        return total
    outputs = lax.map(expert, jnp.arange(E_WIN, dtype=jnp.int32)).reshape(total_slots, tokens.shape[1])
    mixed = jnp.zeros((tokens.shape[0] + 1, tokens.shape[1]), jnp.float32).at[source].add(outputs * weight[:, None])
    mixed = mixed[:tokens.shape[0]].astype(jnp.bfloat16)
    load = jnp.zeros((NEXP,), jnp.float32).at[expert_ids.reshape(-1)].add(jnp.float32(1.0))
    mean_load = jnp.float32(TOKENS * TOPK / NEXP)
    new_bias = bias - 0.05 * (load - mean_load) / jnp.sqrt(mean_load)
    return (mixed, new_bias)
```

```python
import functools
import math

import jax
import jax.numpy as jnp
from jax import lax
from jax.experimental import pallas as pl
from jax.experimental.pallas import tpu as pltpu
from jax.sharding import Mesh
from jax.sharding import PartitionSpec as P

NEXP = 128
TOPK = 8
NWIN = 4
CAP = 16
AXES = ("xl", "y", "xh", "z", "c")
MESH = pl.DeviceIdType.MESH
f32 = jnp.float32
bf16 = jnp.bfloat16


def kernel(
    sizes, mean_load,
    ids_ref, comb_ref, bias_ref, tok_hbm, wg_hbm, wu_hbm, wd_hbm,
    mixed_ref, nb_ref,
    tok, wg, wu, wd, ent, xbuf, part, ret, fin, sw, lsend, lrecv,
    in_sem, ent_ss, fr_ss, fl_ss, x_rs, rr_ss, rl_ss, r_rs, fx_ss, f_rs, l_ss, l_rs,
):
    nxh, nz, nc = sizes
    width = tok.shape[1]
    xl, y = lax.axis_index("xl"), lax.axis_index("y")
    xh, z, c = lax.axis_index("xh"), lax.axis_index("z"), lax.axis_index("c")
    quad, s = lax.div(y, 4), lax.rem(y, 4)
    own = 2 * xl + quad
    mate = 1 - xl

    loads = [
        pltpu.make_async_copy(tok_hbm, tok, in_sem.at[0]),
        pltpu.make_async_copy(wg_hbm, wg, in_sem.at[1]),
        pltpu.make_async_copy(wu_hbm, wu, in_sem.at[2]),
        pltpu.make_async_copy(wd_hbm, wd, in_sem.at[3]),
    ]
    for copy in loads:
        copy.start()

    nx = 2 * nxh
    xi = 2 * xh + xl
    y_peers = [(lax.rem(y + k, 8), {"y": lax.rem(y + k, 8)}) for k in range(1, 8)]
    x_peers = []
    for k in range(1, nx):
        other = lax.rem(xi + k, nx)
        x_peers.append((other, {"xl": lax.rem(other, 2), "xh": lax.div(other, 2)}))
    z_peers = [(lax.rem(z + k, nz), {"z": lax.rem(z + k, nz)}) for k in range(1, nz)]
    c_peers = [(lax.rem(c + k, nc), {"c": lax.rem(c + k, nc)}) for k in range(1, nc)]
    greeted = [where for _, where in y_peers + x_peers + z_peers + c_peers]
    for dy in (-2, -1, 1, 2):
        greeted.append({"xl": mate, "y": lax.rem(y + dy + 8, 8)})
    barrier = pltpu.get_barrier_semaphore()
    for where in greeted:
        pl.semaphore_signal(barrier, inc=1, device_id=where, device_id_type=MESH)

    ids = ids_ref[...]
    comb = comb_ref[...]
    row8 = lax.broadcasted_iota(jnp.int32, (8, 128), 0)
    exps = lax.broadcasted_iota(jnp.int32, (NEXP, 128), 0)
    hit = jnp.zeros((8, 128), f32)
    weight = jnp.zeros((8, 128), f32)
    many = jnp.zeros((NEXP, 128), f32)
    for p in range(TOPK):
        named = ids[p : p + 1, :]
        same = row8 == named
        hit += jnp.where(same, 1.0, 0.0)
        weight += jnp.where(same, comb[p : p + 1, :], 0.0)
        many += jnp.where(exps == named, 1.0, 0.0)
    before = lax.broadcasted_iota(jnp.int32, (128, 128), 0) < lax.broadcasted_iota(
        jnp.int32, (128, 128), 1
    )
    rank = jnp.dot(
        hit.astype(bf16), jnp.where(before, 1.0, 0.0).astype(bf16), preferred_element_type=f32
    )
    slots = lax.broadcasted_iota(jnp.int32, (CAP, 128), 0).astype(f32)
    select, scale = [], []
    for w in range(NWIN):
        there = jnp.where(slots == rank[w : w + 1, :], hit[w : w + 1, :], 0.0)
        select.append(there)
        scale.append(there * weight[w : w + 1, :])
    select = jnp.concatenate(select, axis=0).astype(bf16)
    scale = jnp.concatenate(scale, axis=0)
    high = scale.astype(bf16)
    rest = scale - high.astype(f32)
    middle = rest.astype(bf16)
    low = (rest - middle.astype(f32)).astype(bf16)
    sw[...] = jnp.concatenate([high, middle, low], axis=0)
    counts = lax.dot_general(
        jnp.ones((8, 128), bf16), many.astype(bf16), (((1,), (1,)), ((), ())),
        preferred_element_type=f32,
    )
    lsend[0] = counts

    loads[0].wait()
    step = min(1024, width)
    for at in range(0, width, step):
        rows = jnp.dot(select, tok[:, at : at + step], preferred_element_type=f32)
        ent[:, at : at + step] = rows.astype(bf16)
    xbuf[s + 2, 0:CAP, :] = ent[pl.ds(pl.multiple_of(own * CAP, CAP), CAP), :]

    pl.semaphore_wait(barrier, len(greeted))

    entries = []
    for number, (k, dx) in enumerate(((0, 1), (1, 0), (1, 1))):
        tq = lax.rem(quad + k, 2)
        tx = lax.rem(xl + dx, 2)
        ry = lax.rem(y - 4 * tq + 8, 8)
        o = jnp.where(ry <= 5, ry, ry - 8)
        node = jnp.clip(o, 0, 3)
        w = 2 * tx + tq
        entries.append(
            pltpu.make_async_remote_copy(
                src_ref=ent.at[pl.ds(pl.multiple_of(w * CAP, CAP), CAP)],
                dst_ref=xbuf.at[o + 2, pl.ds(CAP * dx, CAP)],
                send_sem=ent_ss.at[number],
                recv_sem=x_rs.at[o + 2, dx],
                device_id={"xl": tx, "y": 4 * tq + node},
                device_id_type=MESH,
            )
        )

    def forward(i, xr, right):
        block = xbuf.at[i, pl.ds(CAP * xr, CAP)]
        return pltpu.make_async_remote_copy(
            src_ref=block,
            dst_ref=block,
            send_sem=(fr_ss if right else fl_ss).at[i, xr],
            recv_sem=x_rs.at[i, xr],
            device_id={"y": lax.rem(y + (1 if right else 7), 8)},
            device_id_type=MESH,
        )

    entries[0].start()

    @pl.when(s < 3)
    def _():
        forward(s + 2, 0, True).start()

    @pl.when(s > 0)
    def _():
        forward(s + 2, 0, False).start()

    entries[1].start()
    entries[2].start()

    def tell(phase, number, here, peers):
        made = []
        for k, (_, where) in enumerate(peers):
            made.append(
                pltpu.make_async_remote_copy(
                    src_ref=lsend.at[phase],
                    dst_ref=lrecv.at[phase, here],
                    send_sem=l_ss.at[phase, k],
                    recv_sem=l_rs.at[phase, here],
                    device_id=where,
                    device_id_type=MESH,
                )
            )
        return made

    phases = [(y, y_peers), (xi, x_peers), (z, z_peers), (c, c_peers)]

    def tell_all(phase):
        for copy in tell(phase, None, phases[phase][0], phases[phase][1]):
            copy.start()

    def hear_all(phase):
        total = lsend[phase]
        for other, where in phases[phase][1]:
            pltpu.make_async_remote_copy(
                src_ref=lsend.at[phase],
                dst_ref=lrecv.at[phase, other],
                send_sem=l_ss.at[phase, 0],
                recv_sem=l_rs.at[phase, other],
                device_id=where,
                device_id_type=MESH,
            ).wait_recv()
            total = total + lrecv[phase, other]
        return total

    tell_all(0)
    for copy in loads[1:]:
        copy.wait()

    def send_back(i, xr, right):
        block = ret.at[i, pl.ds(CAP * xr, CAP)]
        o = i - 2
        to = lax.rem(y + (1 if right else 7), 8)
        slot = i if right else jnp.where(o == s - 1, 8, i)
        inner = pltpu.make_async_remote_copy(
            src_ref=block,
            dst_ref=ret.at[slot, pl.ds(CAP * xr, CAP)],
            send_sem=(rr_ss if right else rl_ss).at[i, xr],
            recv_sem=r_rs.at[slot, xr],
            device_id={"y": to},
            device_id_type=MESH,
        )
        outer = pltpu.make_async_remote_copy(
            src_ref=block,
            dst_ref=fin.at[own],
            send_sem=(rr_ss if right else rl_ss).at[i, xr],
            recv_sem=f_rs.at[own],
            device_id={
                "xl": lax.rem(xl + xr, 2),
                "y": lax.rem(4 * quad + o + 8, 8),
            },
            device_id_type=MESH,
        )
        return inner, outer

    def arrived(i, xr):
        block = ret.at[i, pl.ds(CAP * xr, CAP)]
        pltpu.make_async_remote_copy(
            src_ref=block, dst_ref=block, send_sem=rr_ss.at[0, xr], recv_sem=r_rs.at[i, xr],
            device_id={"y": lax.rem(y + 1, 8)}, device_id_type=MESH,
        ).wait_recv()

    def to_mate():
        return pltpu.make_async_remote_copy(
            src_ref=ret.at[9, pl.ds(0, CAP)],
            dst_ref=fin.at[own],
            send_sem=fx_ss.at[0],
            recv_sem=f_rs.at[own],
            device_id={"xl": mate},
            device_id_type=MESH,
        )

    last = jnp.maximum(2 * s, 6 - 2 * s)

    def round_(r, carry):
        ol, orr = s - r, s + r
        has_l = (r >= 1) & (ol >= -2)
        has_r = (r >= 1) & (orr <= 5)
        il = jnp.where(has_l, ol, s) + 2
        ir = jnp.where(has_r, orr, s) + 2

        @pl.when(r == 0)
        def _():
            forward(s + 2, 1, True).wait_recv()

            @pl.when(s < 3)
            def _():
                forward(s + 2, 1, True).start()

            @pl.when(s > 0)
            def _():
                forward(s + 2, 1, False).start()

        for xr in (0, 1):

            @pl.when(has_l)
            def _():
                forward(il, xr, True).wait_recv()

                @pl.when(s < 3)
                def _():
                    forward(il, xr, True).start()

            @pl.when(has_r)
            def _():
                forward(ir, xr, False).wait_recv()

                @pl.when(s > 0)
                def _():
                    forward(ir, xr, False).start()

        for phase in range(3):

            @pl.when(r == phase + 1)
            def _():
                lsend[phase + 1] = hear_all(phase)
                tell_all(phase + 1)

        @pl.when(r == 4)
        def _():
            load = hear_all(3)[0:1, :]
            nb_ref[...] = bias_ref[...] - 0.05 * (load - mean_load) / math.sqrt(mean_load)

        @pl.when((r == 0) | has_l | has_r)
        def _():
            rows = jnp.concatenate([xbuf[il], xbuf[ir]], axis=0)
            flat = (((1,), (1,)), ((), ()))
            gate = lax.dot_general(wg[...], rows, flat, preferred_element_type=f32)
            up = lax.dot_general(wu[...], rows, flat, preferred_element_type=f32)
            hidden = (jax.nn.silu(gate) * up).astype(bf16)
            for at in range(0, width, step):
                out = lax.dot_general(
                    hidden, wd[:, at : at + step], (((0,), (0,)), ((), ())),
                    preferred_element_type=f32,
                )
                part[il, :, at : at + step] = out[: 2 * CAP]
                part[ir, :, at : at + step] = out[2 * CAP :]

        for right in (True, False):
            o = r - s if right else 6 - s - r
            valid = (o > s) & (o <= 5) if right else (o < s) & (o >= -2)
            i = o + 2
            first = s == (0 if right else 3)
            end = s == (3 if right else 0)

            for xr in (0, 1):
                span = pl.ds(CAP * xr, CAP)

                @pl.when(valid)
                def _():
                    @pl.when(first)
                    def _():
                        ret[i, span, :] = part[i, span, :].astype(bf16)

                    @pl.when(jnp.logical_not(first))
                    def _():
                        arrived(i, xr)
                        ret[i, span, :] = (part[i, span, :] + ret[i, span, :].astype(f32)).astype(
                            bf16
                        )

                    inner, outer = send_back(i, xr, right)

                    @pl.when(end)
                    def _():
                        outer.start()

                    @pl.when(jnp.logical_not(end))
                    def _():
                        inner.start()

        @pl.when(r == last)
        def _():
            for xr in (1, 0):
                span = pl.ds(CAP * xr, CAP)

                @pl.when(s > 0)
                def _():
                    arrived(s + 2, xr)
                    part[s + 2, span, :] += ret[s + 2, span, :].astype(f32)

                @pl.when(s < 3)
                def _():
                    arrived(8, xr)
                    part[s + 2, span, :] += ret[8, span, :].astype(f32)

                if xr == 1:
                    ret[9, 0:CAP, :] = part[s + 2, span, :].astype(bf16)
                    to_mate().start()
                else:
                    fin[own] = part[s + 2, span, :].astype(bf16)

        return carry

    lax.fori_loop(0, 9, round_, 0)

    for k, dx in ((0, 1), (1, 0), (1, 1)):
        w = 2 * lax.rem(xl + dx, 2) + lax.rem(quad + k, 2)
        pltpu.make_async_remote_copy(
            src_ref=ret.at[9, pl.ds(0, CAP)], dst_ref=fin.at[w], send_sem=fx_ss.at[0],
            recv_sem=f_rs.at[w], device_id={"xl": mate}, device_id_type=MESH,
        ).wait_recv()
    wide = min(512, width)
    for at in range(0, width, wide):
        done = fin[:, :, at : at + wide].reshape(NWIN * CAP, wide)
        done = jnp.concatenate([done, done, done], axis=0)
        mixed_ref[:, at : at + wide] = lax.dot_general(
            sw[...], done, (((0,), (0,)), ((), ())), preferred_element_type=f32
        ).astype(bf16)

    for copy in entries:
        copy.wait_send()
    to_mate().wait_send()
    for phase in range(4):
        for copy in tell(phase, None, phases[phase][0], phases[phase][1]):
            copy.wait_send()

    def drain(i, carry):
        o = i - 2
        for xr in (0, 1):

            @pl.when((s < 3) & (o <= s))
            def _():
                forward(i, xr, True).wait_send()

            @pl.when((s > 0) & (o >= s))
            def _():
                forward(i, xr, False).wait_send()

            @pl.when(o > s)
            def _():
                send_back(i, xr, True)[1].wait_send()

            @pl.when(o < s)
            def _():
                send_back(i, xr, False)[1].wait_send()

        return carry

    lax.fori_loop(0, 8, drain, 0)


def per_device(sizes, tokens, expert_ids, combine, w_gate, w_up, w_down, bias):
    tok_rows, width = tokens.shape
    hidden = w_down.shape[0]
    devices = 16 * math.prod(sizes)
    mean_load = float(tok_rows * devices * TOPK / NEXP)
    vmem = pl.BlockSpec(memory_space=pltpu.VMEM)
    hbm = pl.BlockSpec(memory_space=pl.ANY)
    dma = pltpu.SemaphoreType.DMA
    mixed, new_bias = pl.pallas_call(
        functools.partial(kernel, sizes, mean_load),
        out_shape=(
            jax.ShapeDtypeStruct((tok_rows, width), bf16),
            jax.ShapeDtypeStruct((1, NEXP), f32),
        ),
        in_specs=[vmem, vmem, vmem, hbm, hbm, hbm, hbm],
        out_specs=(vmem, vmem),
        scratch_shapes=[
            pltpu.VMEM((tok_rows, width), bf16),
            pltpu.VMEM((hidden, width), bf16),
            pltpu.VMEM((hidden, width), bf16),
            pltpu.VMEM((hidden, width), bf16),
            pltpu.VMEM((NWIN * CAP, width), bf16),
            pltpu.VMEM((8, 2 * CAP, width), bf16),
            pltpu.VMEM((8, 2 * CAP, width), f32),
            pltpu.VMEM((10, 2 * CAP, width), bf16),
            pltpu.VMEM((NWIN, CAP, width), bf16),
            pltpu.VMEM((3 * NWIN * CAP, 128), bf16),
            pltpu.VMEM((4, 8, 128), f32),
            pltpu.VMEM((4, 8, 8, 128), f32),
            dma((4,)),
            dma((3,)),
            dma((8, 2)),
            dma((8, 2)),
            dma((8, 2)),
            dma((8, 2)),
            dma((8, 2)),
            dma((10, 2)),
            dma((1,)),
            dma((NWIN,)),
            dma((4, 8)),
            dma((4, 8)),
        ],
        compiler_params=pltpu.CompilerParams(
            collective_id=0, has_side_effects=True, vmem_limit_bytes=48 * 1024 * 1024
        ),
        name="moe",
    )(
        expert_ids.T, combine.T, bias.reshape(1, NEXP), tokens, w_gate.T, w_up.T, w_down,
    )
    return mixed, new_bias.reshape(NEXP)


def solution(mesh):
    devices = mesh.devices
    ep, grp = devices.shape
    shape = (2, 8, 4, 8, 2) if (ep, grp) == (16, 64) else (2, 8, 1, 1, grp)
    finer = Mesh(devices.reshape(shape), AXES)
    row = P(AXES, None)
    in_specs = (row, row, row, P(None, ("xl", "y")), P(None, ("xl", "y")), P(("xl", "y"), None), P())
    return jax.shard_map(
        functools.partial(per_device, shape[2:]), mesh=finer, in_specs=in_specs,
        out_specs=(row, P()), check_vma=False,
    )
```

```python
import functools
import math

import jax
import jax.numpy as jnp
from jax import lax
from jax.experimental import pallas as pl
from jax.experimental.pallas import tpu as pltpu
from jax.sharding import Mesh
from jax.sharding import PartitionSpec as P

NEXP = 128
TOPK = 8
NWIN = 4
CAP = 16
PIECES = 4
AXES = ("xl", "y", "xh", "z", "c")
MESH = pl.DeviceIdType.MESH
f32 = jnp.float32
bf16 = jnp.bfloat16


def kernel(
    sizes, mean_load,
    ids_hbm, comb_hbm, bias_hbm, tok_hbm, wg_hbm, wu_hbm, wd_hbm,
    mixed_ref, nb_ref,
    ids_ref, comb_ref, bias_ref, tok, wg, wu, wd, ent, xbuf, part, ret, fin, sw, lsend, lrecv,
    in_sem, ent_ss, fr_ss, fl_ss, x_rs, rr_ss, rl_ss, ro_ss, r_rs, fx_ss, f_rs, l_ss, l_rs, hello,
):
    nxh, nz, nc = sizes
    width = tok.shape[1]
    xl, y = lax.axis_index("xl"), lax.axis_index("y")
    xh, z, c = lax.axis_index("xh"), lax.axis_index("z"), lax.axis_index("c")
    quad, s = lax.div(y, 4), lax.rem(y, 4)
    own = 2 * xl + quad
    mate = 1 - xl

    arrays = (
        (ids_hbm, ids_ref), (comb_hbm, comb_ref), (tok_hbm, tok), (wg_hbm, wg), (wu_hbm, wu),
        (wd_hbm, wd), (bias_hbm, bias_ref),
    )
    loads = [pltpu.make_async_copy(a, b, in_sem.at[k]) for k, (a, b) in enumerate(arrays)]
    for copy in loads:
        copy.start()

    nx = 2 * nxh
    xi = 2 * xh + xl
    y_peers = [(lax.rem(y + k, 8), {"y": lax.rem(y + k, 8)}) for k in range(1, 8)]
    x_peers = []
    for k in range(1, nx):
        other = lax.rem(xi + k, nx)
        x_peers.append((other, {"xl": lax.rem(other, 2), "xh": lax.div(other, 2)}))
    z_peers = [(lax.rem(z + k, nz), {"z": lax.rem(z + k, nz)}) for k in range(1, nz)]
    c_peers = [(lax.rem(c + k, nc), {"c": lax.rem(c + k, nc)}) for k in range(1, nc)]
    greeted = [where for _, where in y_peers] + [{"xl": mate}]
    for dy in (-2, -1, 1, 2):
        greeted.append({"xl": mate, "y": lax.rem(y + dy + 8, 8)})
    barrier = pltpu.get_barrier_semaphore()

    def signal(sem, where):
        pl.semaphore_signal(sem, inc=1, device_id=where, device_id_type=MESH)

    for where in greeted:
        signal(barrier, where)

    mate_at = 2 * xh + mate

    def x_asks(other):
        return (xi > other) & (other != mate_at)

    def x_answers(other):
        return (xi < other) & (other != mate_at)

    one_way = (
        (x_peers, x_asks, x_answers),
        (c_peers, lambda other: c > other, lambda other: c < other),
        (z_peers, lambda other: z < other, lambda other: z > other),
    )

    def count(peers, test):
        total = jnp.int32(0)
        for other, _ in peers:
            total = total + jnp.where(test(other), 1, 0)
        return total

    for peers, asks, _ in one_way:
        for other, where in peers:

            @pl.when(asks(other))
            def _():
                signal(barrier, where)

    loads[0].wait()
    loads[1].wait()
    ids = ids_ref[...]
    comb = comb_ref[...]
    row8 = lax.broadcasted_iota(jnp.int32, (8, 128), 0)
    exps = lax.broadcasted_iota(jnp.int32, (NEXP, 128), 0)
    hit = jnp.zeros((8, 128), f32)
    weight = jnp.zeros((8, 128), f32)
    many = jnp.zeros((NEXP, 128), f32)
    for p in range(TOPK):
        named = ids[p : p + 1, :]
        same = row8 == named
        hit += jnp.where(same, 1.0, 0.0)
        weight += jnp.where(same, comb[p : p + 1, :], 0.0)
        many += jnp.where(exps == named, 1.0, 0.0)
    before = lax.broadcasted_iota(jnp.int32, (128, 128), 0) < lax.broadcasted_iota(
        jnp.int32, (128, 128), 1
    )
    rank = jnp.dot(
        hit.astype(bf16), jnp.where(before, 1.0, 0.0).astype(bf16), preferred_element_type=f32
    )
    slots = lax.broadcasted_iota(jnp.int32, (CAP, 128), 0).astype(f32)
    select, scale = [], []
    for w in range(NWIN):
        there = jnp.where(slots == rank[w : w + 1, :], hit[w : w + 1, :], 0.0)
        select.append(there)
        scale.append(there * weight[w : w + 1, :])
    select = jnp.concatenate(select, axis=0).astype(bf16)
    scale = jnp.concatenate(scale, axis=0)
    high = scale.astype(bf16)
    rest = scale - high.astype(f32)
    middle = rest.astype(bf16)
    low = (rest - middle.astype(f32)).astype(bf16)
    sw[...] = jnp.concatenate([high, middle, low], axis=0)
    counts = lax.dot_general(
        jnp.ones((8, 128), bf16), many.astype(bf16), (((1,), (1,)), ((), ())),
        preferred_element_type=f32,
    )
    lsend[0] = counts

    loads[2].wait()
    step = width // PIECES
    for at in range(0, width, step):
        rows = jnp.dot(select, tok[:, at : at + step], preferred_element_type=f32)
        ent[:, at : at + step] = rows.astype(bf16)
    xbuf[s + 2, 0:CAP, :] = ent[pl.ds(pl.multiple_of(own * CAP, CAP), CAP), :]

    expected = jnp.int32(len(greeted))
    for peers, _, answers in one_way:
        expected = expected + count(peers, answers)
    pl.semaphore_wait(barrier, expected)
    for axis, (peers, _, answers) in enumerate(one_way):
        for other, where in peers:

            @pl.when(answers(other))
            def _():
                signal(hello.at[axis], where)


    entries = []
    for number, (k, dx) in enumerate(((0, 1), (1, 0), (1, 1))):
        tq = lax.rem(quad + k, 2)
        tx = lax.rem(xl + dx, 2)
        ry = lax.rem(y - 4 * tq + 8, 8)
        o = jnp.where(ry <= 5, ry, ry - 8)
        node = jnp.clip(o, 0, 3)
        w = 2 * tx + tq
        entries.append(
            pltpu.make_async_remote_copy(
                src_ref=ent.at[pl.ds(pl.multiple_of(w * CAP, CAP), CAP)],
                dst_ref=xbuf.at[o + 2, pl.ds(CAP * dx, CAP)],
                send_sem=ent_ss.at[number],
                recv_sem=x_rs.at[o + 2, dx],
                device_id={"xl": tx, "y": 4 * tq + node},
                device_id_type=MESH,
            )
        )

    def forward(i, xr, right):
        block = xbuf.at[i, pl.ds(CAP * xr, CAP)]
        return pltpu.make_async_remote_copy(
            src_ref=block,
            dst_ref=block,
            send_sem=(fr_ss if right else fl_ss).at[i],
            recv_sem=x_rs.at[i, xr],
            device_id={"y": lax.rem(y + (1 if right else 7), 8)},
            device_id_type=MESH,
        )

    entries[0].start()

    @pl.when(s < 2)
    def _():
        forward(s + 2, 0, True).start()

    @pl.when(s > 1)
    def _():
        forward(s + 2, 0, False).start()

    @pl.when((s == 1) | (s == 2))
    def _():
        entries[1].start()
        entries[2].start()

    def tell(phase, number, here, peers):
        made = []
        for k, (_, where) in enumerate(peers):
            made.append(
                pltpu.make_async_remote_copy(
                    src_ref=lsend.at[phase],
                    dst_ref=lrecv.at[phase, here],
                    send_sem=l_ss.at[phase],
                    recv_sem=l_rs.at[phase, here],
                    device_id=where,
                    device_id_type=MESH,
                )
            )
        return made

    phases = [(y, y_peers), (xi, x_peers), (c, c_peers), (z, z_peers)]

    def tell_all(phase):
        if phase > 0:
            peers, asks, _ = one_way[phase - 1]
            answers = count(peers, asks)

            @pl.when(answers > 0)
            def _():
                pl.semaphore_wait(hello.at[phase - 1], answers)

        for copy in tell(phase, None, phases[phase][0], phases[phase][1]):
            copy.start()

    def hear_all(phase):
        total = lsend[phase]
        for other, where in phases[phase][1]:
            pltpu.make_async_remote_copy(
                src_ref=lsend.at[phase],
                dst_ref=lrecv.at[phase, other],
                send_sem=l_ss.at[phase],
                recv_sem=l_rs.at[phase, other],
                device_id=where,
                device_id_type=MESH,
            ).wait_recv()
            total = total + lrecv[phase, other]
        return total

    tell_all(0)
    for copy in loads[3:]:
        copy.wait()

    def piece(ref, i, rows, q):
        return ref.at[i, rows, pl.ds(q * step, step)]

    both = pl.ds(0, 2 * CAP)

    def send_on(i, q, right):
        slot = i if right else jnp.where(i - 2 == s - 1, 8, i)
        return pltpu.make_async_remote_copy(
            src_ref=piece(ret, i, both, q),
            dst_ref=piece(ret, slot, both, q),
            send_sem=(rr_ss if right else rl_ss).at[i],
            recv_sem=r_rs.at[slot, q],
            device_id={"y": lax.rem(y + (1 if right else 7), 8)},
            device_id_type=MESH,
        )

    def send_out(i, q, xr):
        return pltpu.make_async_remote_copy(
            src_ref=piece(ret, i, pl.ds(CAP * xr, CAP), q),
            dst_ref=piece(fin, own, pl.ds(0, CAP), q),
            send_sem=ro_ss.at[i],
            recv_sem=f_rs.at[own, q],
            device_id={"xl": lax.rem(xl + xr, 2), "y": lax.rem(4 * quad + i + 6, 8)},
            device_id_type=MESH,
        )

    def arrived(i, q):
        block = piece(ret, i, both, q)
        pltpu.make_async_remote_copy(
            src_ref=block, dst_ref=block, send_sem=rr_ss.at[0], recv_sem=r_rs.at[i, q],
            device_id={"y": lax.rem(y + 1, 8)}, device_id_type=MESH,
        ).wait_recv()

    def to_mate(q):
        return pltpu.make_async_remote_copy(
            src_ref=piece(ret, 9, pl.ds(0, CAP), q),
            dst_ref=piece(fin, own, pl.ds(0, CAP), q),
            send_sem=fx_ss.at[0],
            recv_sem=f_rs.at[own, q],
            device_id={"xl": mate},
            device_id_type=MESH,
        )

    last = jnp.where((s == 0) | (s == 3), 6, 7)

    def line(k):
        return jnp.where(k <= 3, k, jnp.where(k == 6, 1, 9 - k))

    def round_(r, carry):
        ends = (s == 0) | (s == 3)
        both_in = ends & (r == 1)
        a_has = both_in | ((s == 3) & (r >= 2) & (r <= 6)) | ((r >= 1) & (r <= s + 2) & ~ends)
        b_has = both_in | ((s == 0) & (r >= 2) & (r <= 6)) | ((r >= 1) & (r <= 5 - s) & ~ends)
        a_in = jnp.where(r <= s, s - r, r - s - 3)
        b_in = jnp.where(r <= 3 - s, s + r, 9 - s - r)
        a_o = jnp.where(s == 0, -2, jnp.where(s == 3, jnp.where(r == 1, 5, 3 - line(r)), a_in))
        b_o = jnp.where(s == 3, 4, jnp.where(s == 0, jnp.where(r == 1, -1, line(r)), b_in))
        ia = jnp.where(a_has, a_o, s) + 2
        ib = jnp.where(b_has, b_o, s) + 2
        inner = (s == 1) | (s == 2)
        streams = (
            (ia, a_has, (inner & a_has) | ((s == 0) & (r == 1)), (s == 3) & (r == 1)),
            (ib, b_has, (s == 0) & (r == 1), (inner & b_has) | ((s == 3) & (r == 1))),
        )

        @pl.when(r == 0)
        def _():
            forward(s + 2, 1, True).wait_recv()

            @pl.when(s < 2)
            def _():
                forward(s + 2, 1, True).start()

            @pl.when(s > 1)
            def _():
                forward(s + 2, 1, False).start()

            @pl.when((s == 0) | (s == 3))
            def _():
                entries[1].start()
                entries[2].start()

        for i, has, go_right, go_left in streams:
            for xr in (0, 1):

                @pl.when(has)
                def _():
                    forward(i, xr, True).wait_recv()

                @pl.when(go_right)
                def _():
                    forward(i, xr, True).start()

                @pl.when(go_left)
                def _():
                    forward(i, xr, False).start()

        @pl.when((r == 4) & (s == 2))
        def _():
            forward(s + 2, 0, True).start()
            forward(s + 2, 1, True).start()

        @pl.when((r == 4) & (s == 1))
        def _():
            forward(s + 2, 0, False).start()
            forward(s + 2, 1, False).start()

        for phase, when in enumerate((2, 4, 5)):

            @pl.when(r == when)
            def _():
                lsend[phase + 1] = hear_all(phase)
                tell_all(phase + 1)

        @pl.when((r == 0) | a_has | b_has)
        def _():
            rows = jnp.concatenate([xbuf[ia], xbuf[ib]], axis=0)
            flat = (((1,), (1,)), ((), ()))
            gate = lax.dot_general(wg[...], rows, flat, preferred_element_type=f32)
            up = lax.dot_general(wu[...], rows, flat, preferred_element_type=f32)
            hidden = (jax.nn.silu(gate) * up).astype(bf16)
            for at in range(0, width, step):
                out = lax.dot_general(
                    hidden, wd[:, at : at + step], (((0,), (0,)), ((), ())),
                    preferred_element_type=f32,
                )
                part[ia, :, at : at + step] = out[: 2 * CAP]
                part[ib, :, at : at + step] = out[2 * CAP :]

        for q in range(PIECES):
            cols = slice(q * step, (q + 1) * step)
            for right in (True, False):
                at = s if right else 3 - s
                k = r - at
                along = line(k)
                valid = (k >= 2) & (k <= 6) & (along > at)
                o = along if right else 3 - along
                i = o + 2
                first = s == (0 if right else 3)
                end = s == (3 if right else 0)

                @pl.when(valid)
                def _():
                    @pl.when(first)
                    def _():
                        ret[i, :, cols] = part[i, :, cols].astype(bf16)

                    @pl.when(jnp.logical_not(first))
                    def _():
                        arrived(i, q)
                        ret[i, :, cols] = (part[i, :, cols] + ret[i, :, cols].astype(f32)).astype(
                            bf16
                        )

                    @pl.when(end)
                    def _():
                        send_out(i, q, 0).start()
                        send_out(i, q, 1).start()

                    @pl.when(jnp.logical_not(end))
                    def _():
                        send_on(i, q, right).start()

        @pl.when(r == last)
        def _():
            for q in range(PIECES):
                cols = slice(q * step, (q + 1) * step)

                @pl.when(s > 0)
                def _():
                    arrived(s + 2, q)
                    part[s + 2, :, cols] += ret[s + 2, :, cols].astype(f32)

                @pl.when(s < 3)
                def _():
                    arrived(8, q)
                    part[s + 2, :, cols] += ret[8, :, cols].astype(f32)

                ret[9, 0:CAP, cols] = part[s + 2, CAP : 2 * CAP, cols].astype(bf16)
                to_mate(q).start()
                fin[own, :, cols] = part[s + 2, 0:CAP, cols].astype(bf16)

        return carry

    lax.fori_loop(0, 9, round_, 0)

    def drained(ref, i, sem, rows=2 * CAP):
        block = ref.at[i, pl.ds(0, rows)]
        pltpu.make_async_remote_copy(
            src_ref=block, dst_ref=block, send_sem=sem, recv_sem=f_rs.at[0, 0],
            device_id={"xl": mate}, device_id_type=MESH,
        ).wait_send()

    for copy in entries:
        copy.wait_send()
    for phase in range(4):
        told = len(phases[phase][1])
        if told:
            drained(lrecv, phase, l_ss.at[phase], told)

    def drain_rows(i, carry):
        @pl.when((s < 3) & (i - 2 <= s))
        def _():
            drained(xbuf, i, fr_ss.at[i])

        @pl.when((s > 0) & (i - 2 >= s))
        def _():
            drained(xbuf, i, fl_ss.at[i])

        return carry

    lax.fori_loop(0, 8, drain_rows, 0)

    load = hear_all(3)[0:1, :]
    nb_ref[...] = bias_ref[...] - 0.05 * (load - mean_load) / math.sqrt(mean_load)
    for q in range(PIECES):
        cols = slice(q * step, (q + 1) * step)
        for k, dx in ((0, 1), (1, 0), (1, 1)):
            w = 2 * lax.rem(xl + dx, 2) + lax.rem(quad + k, 2)
            pltpu.make_async_remote_copy(
                src_ref=piece(ret, 9, pl.ds(0, CAP), q),
                dst_ref=piece(fin, w, pl.ds(0, CAP), q),
                send_sem=fx_ss.at[0],
                recv_sem=f_rs.at[w, q],
                device_id={"xl": mate},
                device_id_type=MESH,
            ).wait_recv()
        done = fin[:, :, cols].reshape(NWIN * CAP, step)
        done = jnp.concatenate([done, done, done], axis=0)
        mixed_ref[:, cols] = lax.dot_general(
            sw[...], done, (((0,), (0,)), ((), ())), preferred_element_type=f32
        ).astype(bf16)

    drained(ret, 9, fx_ss.at[0], CAP)

    def drain(i, carry):
        o = i - 2

        @pl.when((o > s) & (s < 3))
        def _():
            drained(ret, i, rr_ss.at[i])

        @pl.when((o < s) & (s > 0))
        def _():
            drained(ret, i, rl_ss.at[i])

        @pl.when(((s == 3) & (o > 3)) | ((s == 0) & (o < 0)))
        def _():
            drained(ret, i, ro_ss.at[i])

        return carry

    lax.fori_loop(0, 8, drain, 0)


def per_device(sizes, tokens, expert_ids, combine, w_gate, w_up, w_down, bias):
    tok_rows, width = tokens.shape
    hidden = w_down.shape[0]
    devices = 16 * math.prod(sizes)
    mean_load = float(tok_rows * devices * TOPK / NEXP)
    vmem = pl.BlockSpec(memory_space=pltpu.VMEM)
    hbm = pl.BlockSpec(memory_space=pl.ANY)
    dma = pltpu.SemaphoreType.DMA
    mixed, new_bias = pl.pallas_call(
        functools.partial(kernel, sizes, mean_load),
        out_shape=(
            jax.ShapeDtypeStruct((tok_rows, width), bf16),
            jax.ShapeDtypeStruct((1, NEXP), f32),
        ),
        in_specs=[hbm] * 7,
        out_specs=(vmem, vmem),
        scratch_shapes=[
            pltpu.VMEM((TOPK, tok_rows), jnp.int32),
            pltpu.VMEM((TOPK, tok_rows), f32),
            pltpu.VMEM((1, NEXP), f32),
            pltpu.VMEM((tok_rows, width), bf16),
            pltpu.VMEM((hidden, width), bf16),
            pltpu.VMEM((hidden, width), bf16),
            pltpu.VMEM((hidden, width), bf16),
            pltpu.VMEM((NWIN * CAP, width), bf16),
            pltpu.VMEM((8, 2 * CAP, width), bf16),
            pltpu.VMEM((8, 2 * CAP, width), f32),
            pltpu.VMEM((10, 2 * CAP, width), bf16),
            pltpu.VMEM((NWIN, CAP, width), bf16),
            pltpu.VMEM((3 * NWIN * CAP, 128), bf16),
            pltpu.VMEM((4, 8, 128), f32),
            pltpu.VMEM((4, 8, 8, 128), f32),
            dma((7,)),
            dma((3,)),
            dma((8,)),
            dma((8,)),
            dma((8, 2)),
            dma((8,)),
            dma((8,)),
            dma((8,)),
            dma((10, PIECES)),
            dma((1,)),
            dma((NWIN, PIECES)),
            dma((4,)),
            dma((4, 8)),
            pltpu.SemaphoreType.REGULAR((3,)),
        ],
        compiler_params=pltpu.CompilerParams(
            collective_id=0, has_side_effects=True, vmem_limit_bytes=67043328
        ),
        name="moe",
    )(
        expert_ids.T, combine.T, bias.reshape(1, NEXP), tokens, w_gate.T, w_up.T, w_down,
    )
    return mixed, new_bias.reshape(NEXP)


def solution(mesh):
    devices = mesh.devices
    ep, grp = devices.shape
    shape = (2, 8, 4, 8, 2) if (ep, grp) == (16, 64) else (2, 8, 1, 1, grp)
    finer = Mesh(devices.reshape(shape), AXES)
    row = P(AXES, None)
    in_specs = (row, row, row, P(None, ("xl", "y")), P(None, ("xl", "y")), P(("xl", "y"), None), P())
    return jax.shard_map(
        functools.partial(per_device, shape[2:]), mesh=finer, in_specs=in_specs,
        out_specs=(row, P()), check_vma=False,
    )
```

```python
import functools
import math

import jax
import jax.numpy as jnp
from jax import lax
from jax.experimental import pallas as pl
from jax.experimental.pallas import tpu as pltpu
from jax.sharding import Mesh
from jax.sharding import PartitionSpec as P

NEXP = 128
TOPK = 8
NWIN = 4
CAP = 16
PIECES = 4
AXES = ("xl", "y", "xh", "z", "c")
MESH = pl.DeviceIdType.MESH
f32 = jnp.float32
bf16 = jnp.bfloat16


def kernel(
    sizes,
    ids_hbm, comb_hbm, tok_hbm, wg_hbm, wu_hbm, wd_hbm,
    fin_hbm, sw_hbm, load_hbm,
    ids_ref, comb_ref, load_ref, tok, wg, wu, wd, ent, xbuf, part, ret, fin, sw, lsend, lrecv,
    in_sem, ent_ss, fr_ss, fl_ss, x_rs, rr_ss, rl_ss, ro_ss, r_rs, fx_ss, f_rs, l_ss, l_rs, hello, out_sem,
):
    nxh, nz, nc = sizes
    width = tok.shape[1]
    xl, y = lax.axis_index("xl"), lax.axis_index("y")
    xh, z, c = lax.axis_index("xh"), lax.axis_index("z"), lax.axis_index("c")
    quad, s = lax.div(y, 4), lax.rem(y, 4)
    own = 2 * xl + quad
    mate = 1 - xl

    arrays = (
        (ids_hbm, ids_ref), (comb_hbm, comb_ref), (tok_hbm, tok), (wg_hbm, wg), (wu_hbm, wu),
        (wd_hbm, wd),
    )
    loads = [pltpu.make_async_copy(a, b, in_sem.at[k]) for k, (a, b) in enumerate(arrays)]
    for copy in loads:
        copy.start()

    nx = 2 * nxh
    xi = 2 * xh + xl
    y_peers = [(lax.rem(y + k, 8), {"y": lax.rem(y + k, 8)}) for k in range(1, 8)]
    x_peers = []
    for k in range(1, nx):
        other = lax.rem(xi + k, nx)
        x_peers.append((other, {"xl": lax.rem(other, 2), "xh": lax.div(other, 2)}))
    z_peers = [(lax.rem(z + k, nz), {"z": lax.rem(z + k, nz)}) for k in range(1, nz)]
    c_peers = [(lax.rem(c + k, nc), {"c": lax.rem(c + k, nc)}) for k in range(1, nc)]
    greeted = [where for _, where in y_peers] + [{"xl": mate}]
    for dy in (-2, -1, 1, 2):
        greeted.append({"xl": mate, "y": lax.rem(y + dy + 8, 8)})
    barrier = pltpu.get_barrier_semaphore()

    def signal(sem, where):
        pl.semaphore_signal(sem, inc=1, device_id=where, device_id_type=MESH)

    for where in greeted:
        signal(barrier, where)

    mate_at = 2 * xh + mate

    def x_asks(other):
        return (xi > other) & (other != mate_at)

    def x_answers(other):
        return (xi < other) & (other != mate_at)

    one_way = (
        (x_peers, x_asks, x_answers),
        (c_peers, lambda other: c > other, lambda other: c < other),
        (z_peers, lambda other: z < other, lambda other: z > other),
    )

    def count(peers, test):
        total = jnp.int32(0)
        for other, _ in peers:
            total = total + jnp.where(test(other), 1, 0)
        return total

    for peers, asks, _ in one_way:
        for other, where in peers:

            @pl.when(asks(other))
            def _():
                signal(barrier, where)

    loads[0].wait()
    loads[1].wait()
    ids = ids_ref[...]
    comb = comb_ref[...]
    row8 = lax.broadcasted_iota(jnp.int32, (8, 128), 0)
    exps = lax.broadcasted_iota(jnp.int32, (NEXP, 128), 0)
    hit = jnp.zeros((8, 128), f32)
    weight = jnp.zeros((8, 128), f32)
    many = jnp.zeros((NEXP, 128), f32)
    for p in range(TOPK):
        named = ids[p : p + 1, :]
        same = row8 == named
        hit += jnp.where(same, 1.0, 0.0)
        weight += jnp.where(same, comb[p : p + 1, :], 0.0)
        many += jnp.where(exps == named, 1.0, 0.0)
    before = lax.broadcasted_iota(jnp.int32, (128, 128), 0) < lax.broadcasted_iota(
        jnp.int32, (128, 128), 1
    )
    rank = jnp.dot(
        hit.astype(bf16), jnp.where(before, 1.0, 0.0).astype(bf16), preferred_element_type=f32
    )
    slots = lax.broadcasted_iota(jnp.int32, (CAP, 128), 0).astype(f32)
    select, scale = [], []
    for w in range(NWIN):
        there = jnp.where(slots == rank[w : w + 1, :], hit[w : w + 1, :], 0.0)
        select.append(there)
        scale.append(there * weight[w : w + 1, :])
    select = jnp.concatenate(select, axis=0).astype(bf16)
    scale = jnp.concatenate(scale, axis=0)
    high = scale.astype(bf16)
    rest = scale - high.astype(f32)
    middle = rest.astype(bf16)
    low = (rest - middle.astype(f32)).astype(bf16)
    sw[...] = jnp.concatenate([high, middle, low], axis=0)
    sw_out = pltpu.make_async_copy(sw, sw_hbm, out_sem.at[0])
    load_out = pltpu.make_async_copy(load_ref, load_hbm, out_sem.at[1])
    counts = lax.dot_general(
        jnp.ones((8, 128), bf16), many.astype(bf16), (((1,), (1,)), ((), ())),
        preferred_element_type=f32,
    )
    lsend[0] = counts

    loads[2].wait()
    step = width // PIECES
    for at in range(0, width, step):
        rows = jnp.dot(select, tok[:, at : at + step], preferred_element_type=f32)
        ent[:, at : at + step] = rows.astype(bf16)
    xbuf[s + 2, 0:CAP, :] = ent[pl.ds(pl.multiple_of(own * CAP, CAP), CAP), :]

    expected = jnp.int32(len(greeted))
    for peers, _, answers in one_way:
        expected = expected + count(peers, answers)
    pl.semaphore_wait(barrier, expected)
    for axis, (peers, _, answers) in enumerate(one_way):
        for other, where in peers:

            @pl.when(answers(other))
            def _():
                signal(hello.at[axis], where)


    entries = []
    for number, (k, dx) in enumerate(((0, 1), (1, 0), (1, 1))):
        tq = lax.rem(quad + k, 2)
        tx = lax.rem(xl + dx, 2)
        ry = lax.rem(y - 4 * tq + 8, 8)
        o = jnp.where(ry <= 5, ry, ry - 8)
        node = jnp.clip(o, 0, 3)
        w = 2 * tx + tq
        entries.append(
            pltpu.make_async_remote_copy(
                src_ref=ent.at[pl.ds(pl.multiple_of(w * CAP, CAP), CAP)],
                dst_ref=xbuf.at[o + 2, pl.ds(CAP * dx, CAP)],
                send_sem=ent_ss.at[number],
                recv_sem=x_rs.at[o + 2, dx],
                device_id={"xl": tx, "y": 4 * tq + node},
                device_id_type=MESH,
            )
        )

    def forward(i, xr, right):
        block = xbuf.at[i, pl.ds(CAP * xr, CAP)]
        return pltpu.make_async_remote_copy(
            src_ref=block,
            dst_ref=block,
            send_sem=(fr_ss if right else fl_ss).at[i],
            recv_sem=x_rs.at[i, xr],
            device_id={"y": lax.rem(y + (1 if right else 7), 8)},
            device_id_type=MESH,
        )

    entries[0].start()

    @pl.when(s < 2)
    def _():
        forward(s + 2, 0, True).start()

    @pl.when(s > 1)
    def _():
        forward(s + 2, 0, False).start()

    @pl.when((s == 1) | (s == 2))
    def _():
        entries[1].start()
        entries[2].start()

    def tell(phase, number, here, peers):
        made = []
        for k, (_, where) in enumerate(peers):
            made.append(
                pltpu.make_async_remote_copy(
                    src_ref=lsend.at[phase],
                    dst_ref=lrecv.at[phase, here],
                    send_sem=l_ss.at[phase],
                    recv_sem=l_rs.at[phase, here],
                    device_id=where,
                    device_id_type=MESH,
                )
            )
        return made

    phases = [(y, y_peers), (xi, x_peers), (c, c_peers), (z, z_peers)]

    def tell_all(phase):
        if phase > 0:
            peers, asks, _ = one_way[phase - 1]
            answers = count(peers, asks)

            @pl.when(answers > 0)
            def _():
                pl.semaphore_wait(hello.at[phase - 1], answers)

        for copy in tell(phase, None, phases[phase][0], phases[phase][1]):
            copy.start()

    def hear_all(phase):
        total = lsend[phase]
        for other, where in phases[phase][1]:
            pltpu.make_async_remote_copy(
                src_ref=lsend.at[phase],
                dst_ref=lrecv.at[phase, other],
                send_sem=l_ss.at[phase],
                recv_sem=l_rs.at[phase, other],
                device_id=where,
                device_id_type=MESH,
            ).wait_recv()
            total = total + lrecv[phase, other]
        return total

    tell_all(0)
    for copy in loads[3:]:
        copy.wait()

    def piece(ref, i, rows, q):
        return ref.at[i, rows, pl.ds(q * step, step)]

    both = pl.ds(0, 2 * CAP)

    def send_on(i, q, right):
        slot = i if right else jnp.where(i - 2 == s - 1, 8, i)
        return pltpu.make_async_remote_copy(
            src_ref=piece(ret, i, both, q),
            dst_ref=piece(ret, slot, both, q),
            send_sem=(rr_ss if right else rl_ss).at[i],
            recv_sem=r_rs.at[slot, q],
            device_id={"y": lax.rem(y + (1 if right else 7), 8)},
            device_id_type=MESH,
        )

    def send_out(i, q, xr):
        return pltpu.make_async_remote_copy(
            src_ref=piece(ret, i, pl.ds(CAP * xr, CAP), q),
            dst_ref=piece(fin, own, pl.ds(0, CAP), q),
            send_sem=ro_ss.at[i],
            recv_sem=f_rs.at[own, q],
            device_id={"xl": lax.rem(xl + xr, 2), "y": lax.rem(4 * quad + i + 6, 8)},
            device_id_type=MESH,
        )

    def arrived(i, q):
        block = piece(ret, i, both, q)
        pltpu.make_async_remote_copy(
            src_ref=block, dst_ref=block, send_sem=rr_ss.at[0], recv_sem=r_rs.at[i, q],
            device_id={"y": lax.rem(y + 1, 8)}, device_id_type=MESH,
        ).wait_recv()

    def to_mate(q):
        return pltpu.make_async_remote_copy(
            src_ref=piece(ret, 9, pl.ds(0, CAP), q),
            dst_ref=piece(fin, own, pl.ds(0, CAP), q),
            send_sem=fx_ss.at[0],
            recv_sem=f_rs.at[own, q],
            device_id={"xl": mate},
            device_id_type=MESH,
        )

    last = jnp.where((s == 0) | (s == 3), 6, 7)

    def line(k):
        return jnp.where(k <= 3, k, jnp.where(k == 6, 1, 9 - k))

    def round_(r, carry):
        ends = (s == 0) | (s == 3)
        both_in = ends & (r == 1)
        a_has = both_in | ((s == 3) & (r >= 2) & (r <= 6)) | ((r >= 1) & (r <= s + 2) & ~ends)
        b_has = both_in | ((s == 0) & (r >= 2) & (r <= 6)) | ((r >= 1) & (r <= 5 - s) & ~ends)
        a_in = jnp.where(r <= s, s - r, r - s - 3)
        b_in = jnp.where(r <= 3 - s, s + r, 9 - s - r)
        a_o = jnp.where(s == 0, -2, jnp.where(s == 3, jnp.where(r == 1, 5, 3 - line(r)), a_in))
        b_o = jnp.where(s == 3, 4, jnp.where(s == 0, jnp.where(r == 1, -1, line(r)), b_in))
        ia = jnp.where(a_has, a_o, s) + 2
        ib = jnp.where(b_has, b_o, s) + 2
        inner = (s == 1) | (s == 2)
        streams = (
            (ia, a_has, (inner & a_has) | ((s == 0) & (r == 1)), (s == 3) & (r == 1)),
            (ib, b_has, (s == 0) & (r == 1), (inner & b_has) | ((s == 3) & (r == 1))),
        )

        @pl.when(r == 0)
        def _():
            forward(s + 2, 1, True).wait_recv()

            @pl.when(s < 2)
            def _():
                forward(s + 2, 1, True).start()

            @pl.when(s > 1)
            def _():
                forward(s + 2, 1, False).start()

            @pl.when((s == 0) | (s == 3))
            def _():
                entries[1].start()
                entries[2].start()

        for i, has, go_right, go_left in streams:
            for xr in (0, 1):

                @pl.when(has)
                def _():
                    forward(i, xr, True).wait_recv()

                @pl.when(go_right)
                def _():
                    forward(i, xr, True).start()

                @pl.when(go_left)
                def _():
                    forward(i, xr, False).start()

        @pl.when((r == 4) & (s == 2))
        def _():
            forward(s + 2, 0, True).start()
            forward(s + 2, 1, True).start()

        @pl.when((r == 4) & (s == 1))
        def _():
            forward(s + 2, 0, False).start()
            forward(s + 2, 1, False).start()

        for phase, when in enumerate((2, 4, 5)):

            @pl.when(r == when)
            def _():
                lsend[phase + 1] = hear_all(phase)
                tell_all(phase + 1)

        @pl.when((r == 0) | a_has | b_has)
        def _():
            rows = jnp.concatenate([xbuf[ia], xbuf[ib]], axis=0)
            flat = (((1,), (1,)), ((), ()))
            gate = lax.dot_general(wg[...], rows, flat, preferred_element_type=f32)
            up = lax.dot_general(wu[...], rows, flat, preferred_element_type=f32)
            hidden = (jax.nn.silu(gate) * up).astype(bf16)
            for at in range(0, width, step):
                out = lax.dot_general(
                    hidden, wd[:, at : at + step], (((0,), (0,)), ((), ())),
                    preferred_element_type=f32,
                )
                part[ia, :, at : at + step] = out[: 2 * CAP]
                part[ib, :, at : at + step] = out[2 * CAP :]

        def sums(right, turn):
            at = s if right else 3 - s
            k = r - at
            along = line(k)
            valid = (k >= 2) & (k <= 6) & (along > at) & turn
            i = (along if right else 3 - along) + 2
            first = s == (0 if right else 3)
            end = s == (3 if right else 0)

            @pl.when(valid)
            def _():
                for q in range(PIECES):
                    cols = slice(q * step, (q + 1) * step)

                    @pl.when(first)
                    def _():
                        ret[i, :, cols] = part[i, :, cols].astype(bf16)

                    @pl.when(jnp.logical_not(first))
                    def _():
                        arrived(i, q)
                        ret[i, :, cols] = (part[i, :, cols] + ret[i, :, cols].astype(f32)).astype(
                            bf16
                        )

                    @pl.when(end)
                    def _():
                        send_out(i, q, 0).start()
                        send_out(i, q, 1).start()

                    @pl.when(jnp.logical_not(end))
                    def _():
                        send_on(i, q, right).start()

        sums(False, s >= 2)
        sums(True, s >= 0)
        sums(False, s < 2)

        @pl.when(r == last)
        def _():
            for q in range(PIECES):
                cols = slice(q * step, (q + 1) * step)

                @pl.when(s > 0)
                def _():
                    arrived(s + 2, q)
                    part[s + 2, :, cols] += ret[s + 2, :, cols].astype(f32)

                @pl.when(s < 3)
                def _():
                    arrived(8, q)
                    part[s + 2, :, cols] += ret[8, :, cols].astype(f32)

                ret[9, 0:CAP, cols] = part[s + 2, CAP : 2 * CAP, cols].astype(bf16)
                to_mate(q).start()
                fin[own, :, cols] = part[s + 2, 0:CAP, cols].astype(bf16)

        return carry

    lax.fori_loop(0, 9, round_, 0)

    def drained(ref, i, sem, rows=2 * CAP):
        block = ref.at[i, pl.ds(0, rows)]
        pltpu.make_async_remote_copy(
            src_ref=block, dst_ref=block, send_sem=sem, recv_sem=f_rs.at[0, 0],
            device_id={"xl": mate}, device_id_type=MESH,
        ).wait_send()

    for copy in entries:
        copy.wait_send()
    for phase in range(4):
        told = len(phases[phase][1])
        if told:
            drained(lrecv, phase, l_ss.at[phase], told)

    def drain_rows(i, carry):
        @pl.when((s < 3) & (i - 2 <= s))
        def _():
            drained(xbuf, i, fr_ss.at[i])

        @pl.when((s > 0) & (i - 2 >= s))
        def _():
            drained(xbuf, i, fl_ss.at[i])

        return carry

    lax.fori_loop(0, 8, drain_rows, 0)

    sw_out.start()
    load_ref[...] = hear_all(3)
    load_out.start()

    def fin_out(q):
        cols = pl.ds(q * step, step)
        return pltpu.make_async_copy(fin.at[:, :, cols], fin_hbm.at[:, :, cols], out_sem.at[2 + q])

    for q in range(PIECES):
        for k, dx in ((0, 1), (1, 0), (1, 1)):
            w = 2 * lax.rem(xl + dx, 2) + lax.rem(quad + k, 2)
            pltpu.make_async_remote_copy(
                src_ref=piece(ret, 9, pl.ds(0, CAP), q),
                dst_ref=piece(fin, w, pl.ds(0, CAP), q),
                send_sem=fx_ss.at[0],
                recv_sem=f_rs.at[w, q],
                device_id={"xl": mate},
                device_id_type=MESH,
            ).wait_recv()
        fin_out(q).start()

    drained(ret, 9, fx_ss.at[0], CAP)

    def drain(i, carry):
        o = i - 2

        @pl.when((o > s) & (s < 3))
        def _():
            drained(ret, i, rr_ss.at[i])

        @pl.when((o < s) & (s > 0))
        def _():
            drained(ret, i, rl_ss.at[i])

        @pl.when(((s == 3) & (o > 3)) | ((s == 0) & (o < 0)))
        def _():
            drained(ret, i, ro_ss.at[i])

        return carry

    lax.fori_loop(0, 8, drain, 0)
    sw_out.wait()
    load_out.wait()
    for q in range(PIECES):
        fin_out(q).wait()


def finish(mean_load, fin_ref, sw_ref, load_ref, bias_ref, mixed_hbm, nb_ref, out, out_sem):
    width = out.shape[1]
    step = width // PIECES
    copies = []
    for q in range(PIECES):
        cols = slice(q * step, (q + 1) * step)
        done = fin_ref[:, :, cols].reshape(NWIN * CAP, step)
        done = jnp.concatenate([done, done, done], axis=0)
        out[:, cols] = lax.dot_general(
            sw_ref[...], done, (((0,), (0,)), ((), ())), preferred_element_type=f32
        ).astype(bf16)
        span = pl.ds(q * step, step)
        copies.append(
            pltpu.make_async_copy(out.at[:, span], mixed_hbm.at[:, span], out_sem.at[q])
        )
        copies[-1].start()
    nb_ref[...] = bias_ref[...] - 0.05 * (load_ref[0:1, :] - mean_load) / math.sqrt(mean_load)
    for copy in copies:
        copy.wait()


def per_device(sizes, tokens, expert_ids, combine, w_gate, w_up, w_down, bias):
    tok_rows, width = tokens.shape
    hidden = w_down.shape[0]
    devices = 16 * math.prod(sizes)
    mean_load = float(tok_rows * devices * TOPK / NEXP)
    hbm = pl.BlockSpec(memory_space=pl.ANY)
    dma = pltpu.SemaphoreType.DMA
    fin, sw, load = pl.pallas_call(
        functools.partial(kernel, sizes),
        out_shape=(
            jax.ShapeDtypeStruct((NWIN, CAP, width), bf16),
            jax.ShapeDtypeStruct((3 * NWIN * CAP, tok_rows), bf16),
            jax.ShapeDtypeStruct((8, NEXP), f32),
        ),
        in_specs=[hbm] * 6,
        out_specs=(hbm, hbm, hbm),
        scratch_shapes=[
            pltpu.VMEM((TOPK, tok_rows), jnp.int32),
            pltpu.VMEM((TOPK, tok_rows), f32),
            pltpu.VMEM((8, NEXP), f32),
            pltpu.VMEM((tok_rows, width), bf16),
            pltpu.VMEM((hidden, width), bf16),
            pltpu.VMEM((hidden, width), bf16),
            pltpu.VMEM((hidden, width), bf16),
            pltpu.VMEM((NWIN * CAP, width), bf16),
            pltpu.VMEM((8, 2 * CAP, width), bf16),
            pltpu.VMEM((8, 2 * CAP, width), f32),
            pltpu.VMEM((10, 2 * CAP, width), bf16),
            pltpu.VMEM((NWIN, CAP, width), bf16),
            pltpu.VMEM((3 * NWIN * CAP, 128), bf16),
            pltpu.VMEM((4, 8, 128), f32),
            pltpu.VMEM((4, 8, 8, 128), f32),
            dma((6,)),
            dma((3,)),
            dma((8,)),
            dma((8,)),
            dma((8, 2)),
            dma((8,)),
            dma((8,)),
            dma((8,)),
            dma((10, PIECES)),
            dma((1,)),
            dma((NWIN, PIECES)),
            dma((4,)),
            dma((4, 8)),
            pltpu.SemaphoreType.REGULAR((3,)),
            dma((2 + PIECES,)),
        ],
        compiler_params=pltpu.CompilerParams(
            collective_id=0, has_side_effects=True, vmem_limit_bytes=67043328
        ),
        name="moe",
    )(
        expert_ids.T, combine.T, tokens, w_gate.T, w_up.T, w_down,
    )
    vmem = pl.BlockSpec(memory_space=pltpu.VMEM)
    mixed, new_bias = pl.pallas_call(
        functools.partial(finish, mean_load),
        out_shape=(
            jax.ShapeDtypeStruct((tok_rows, width), bf16),
            jax.ShapeDtypeStruct((1, NEXP), f32),
        ),
        in_specs=[vmem] * 4,
        out_specs=(hbm, vmem),
        scratch_shapes=[pltpu.VMEM((tok_rows, width), bf16), dma((PIECES,))],
        name="finish",
    )(fin, sw, load, bias.reshape(1, NEXP))
    return mixed, new_bias.reshape(NEXP)


def solution(mesh):
    devices = mesh.devices
    ep, grp = devices.shape
    shape = (2, 8, 4, 8, 2) if (ep, grp) == (16, 64) else (2, 8, 1, 1, grp)
    finer = Mesh(devices.reshape(shape), AXES)
    row = P(AXES, None)
    in_specs = (row, row, row, P(None, ("xl", "y")), P(None, ("xl", "y")), P(("xl", "y"), None), P())
    return jax.shard_map(
        functools.partial(per_device, shape[2:]), mesh=finer, in_specs=in_specs,
        out_specs=(row, P()), check_vma=False,
    )
```
